32 devices in a mesh: dp: 8 (over z, y), tensor: 4 (over x, core).
Axes of the slice: x: 2, y: 2, z: 4, core: 2. Of those that a mesh axis runs over, the one named last changes fastest.
Arguments:
- hidden: bfloat16 [2048, 18432], P('dp', 'tensor'), may hold values from -6 to 6
- down_weight: bfloat16 [18432, 4608], P('tensor', 'dp'), may hold values from -0.046875 to 0.046875
- residual: bfloat16 [2048, 4608], P('dp'), may hold values from -6 to 6
- post_gain: float32 [4608], replicated, may hold values from 0.5 to 1.5
- pre_gain: float32 [4608], replicated, may hold values from 0.5 to 1.5
- cast_scale: float32 [1], replicated, may hold values from 100 to 400
- amax_history: float32 [3, 1024], replicated, may hold values from 0.25 to 4
Outputs:
- cast_out: bfloat16 [2048, 4608], P('dp')
- residual_out: bfloat16 [2048, 4608], P('dp')
- peaks: float32 [3], replicated
- new_history: float32 [3, 1024], replicated
- new_scales: float32 [3], replicated
The draws below stay inside these ranges and needn't reach their ends.
All inputs are finite; a program needn't handle non-finite values.
Results may differ from the reference program's by a relative error of at most 0.012.
Values may be sent and summed in bfloat16 or wider, within the bound.
A program may use at most 128 MiB of HBM per device.

```python
import math
import jax
import jax.numpy as jnp
from jax import lax

D = 4608
FF_WIN = 18432
HIST = 1024
FF_DEV = 4608
TOKENS = 2048


def block_scale(key, shape, split, low, top_value):
    gain, own = 1.0, jax.random.fold_in(key, 6)
    for dim, shards_of in split:
        heights = jnp.exp(jax.random.uniform(jax.random.fold_in(own, dim), (shards_of,), jnp.float32, low / len(split), top_value / len(split)))
        gain = gain * jnp.repeat(heights, shape[dim] // shards_of).reshape([-1 if axis == dim else 1 for axis in range(len(shape))])
    return gain


def centred(own_key, dims, scale, most, pieces=(), kind=jnp.bfloat16):
    loudness = block_scale(own_key, dims, pieces, -0.22, 0.18) if pieces else 1.0
    array = jax.random.normal(own_key, dims, jnp.float32) * scale * loudness
    return jnp.minimum(jnp.maximum(array, -most), most).astype(kind)


def setup_inputs(seed: int = 0) -> dict:
    key_list = jax.random.split(jax.random.key(seed), 8)
    hidden = centred(key_list[0], (TOKENS, FF_WIN), 1.0, 6.0, ((0, 8), (1, 4)))
    down_weight = centred(key_list[1], (FF_WIN, D), FF_WIN ** -0.5, 0.046875, ((0, 4), (1, 8)))
    residual = centred(key_list[2], (TOKENS, D), 1.0, 6.0, ((0, 8),))
    post_gain = jnp.clip(1.0 + 0.1 * jax.random.normal(key_list[3], (D,), jnp.float32), 0.5, 1.5)
    pre_gain = jnp.clip(1.0 + 0.1 * jax.random.normal(key_list[4], (D,), jnp.float32), 0.5, 1.5)
    cast_scale = jnp.clip(jnp.exp(jax.random.uniform(key_list[5], (1,), jnp.float32, math.log(100.0), math.log(400.0))), 100.0, 400.0)
    amax_history = jnp.clip(jnp.exp(jax.random.uniform(key_list[6], (3, HIST), jnp.float32, math.log(0.25), math.log(4.0))), 0.25, 4.0)
    return dict(hidden=hidden, down_weight=down_weight, residual=residual, post_gain=post_gain, pre_gain=pre_gain, cast_scale=cast_scale, amax_history=amax_history)


norm_epsilon = 1e-06
float_limit = 448.0

def rms_norm(values, gain_vector):
    return values * lax.rsqrt(lax.optimization_barrier(jnp.mean(values * values, axis=-1, keepdims=True)) + norm_epsilon) * gain_vector

def reference(hidden, down_weight, residual, post_gain, pre_gain, cast_scale, amax_history):
    summed = jnp.zeros((hidden.shape[0], down_weight.shape[1]), jnp.float32)
    for shard_index in range(FF_WIN // FF_DEV):
        first = shard_index * FF_DEV
        term = jnp.dot(hidden[:, first:first + FF_DEV], down_weight[first:first + FF_DEV, :], preferred_element_type=jnp.float32)
        term = lax.optimization_barrier(term.astype(jnp.bfloat16)).astype(jnp.float32)
        summed = summed + term
    stream = residual.astype(jnp.float32) + rms_norm(summed, post_gain)
    normed = rms_norm(stream, pre_gain)
    stale_scale = cast_scale[0]
    cast_out = (jnp.clip(normed * stale_scale, -float_limit, float_limit) / stale_scale).astype(jnp.bfloat16)
    peak_values = jnp.stack([jnp.max(jnp.abs(summed)), jnp.max(jnp.abs(stream)), jnp.max(jnp.abs(normed))]).astype(jnp.float32)
    new_history = jnp.concatenate([peak_values[:, None], amax_history[:, :-1]], axis=1)
    new_scales = float_limit / jnp.maximum(lax.optimization_barrier(jnp.max(new_history, axis=1)), 1.0)
    return (cast_out, stream.astype(jnp.bfloat16), peak_values, new_history, new_scales)
```

```python
import functools

import jax
import jax.numpy as jnp
from jax import lax
from jax.experimental import pallas as pl
from jax.experimental.pallas import tpu as pltpu
from jax.sharding import PartitionSpec as P

MESH = pl.DeviceIdType.MESH
norm_epsilon = 1e-06
float_limit = 448.0
CHUNKS = 2


def rms_norm(values, gain_vector):
    return (
        values
        * lax.rsqrt(jnp.mean(values * values, axis=-1, keepdims=True) + norm_epsilon)
        * gain_vector
    )


def factor(mesh):
    devices = mesh.devices
    count = devices.shape[0]
    coords = [tuple(devices[i, 0].coords) for i in range(count)]
    inner = 1
    if count > 1:
        axis = [p != q for p, q in zip(coords[0], coords[1])].index(True)
        while inner < count and all(
            p == q for k, (p, q) in enumerate(zip(coords[0], coords[inner])) if k != axis
        ):
            inner += 1
    outer = count // inner
    if outer >= inner:
        return (outer, inner), (inner, 1)
    return (inner, 1), (outer, inner)


def project_kernel(dims, hid, wei, out, abuf, wbuf, pbuf, rbuf, sbuf, srec, gbuf,
                   loc_sem, a_send, a_recv, w_send, w_recv, p_send, p_recv,
                   s_send, s_recv, g_send, g_recv):
    (na, sa), (nw, sw), nt, half, rr = dims
    d = lax.axis_index("dp")
    t = lax.axis_index("tensor")
    a = lax.rem(lax.div(d, sa), na)
    w = lax.rem(lax.div(d, sw), nw)

    def dev(a_, w_, t_):
        return (a_ * sa + w_ * sw, t_)

    def copy(src, dst, ss, rs, to):
        return pltpu.make_async_remote_copy(
            src_ref=src, dst_ref=dst, send_sem=ss, recv_sem=rs,
            device_id=to, device_id_type=MESH)

    barrier = pltpu.get_barrier_semaphore()
    for o in range(1, na):
        pl.semaphore_signal(barrier, inc=1, device_id=dev(lax.rem(a + o, na), w, t), device_id_type=MESH)
    for o in range(1, nw):
        pl.semaphore_signal(barrier, inc=1, device_id=dev(a, lax.rem(w + o, nw), t), device_id_type=MESH)
    for o in range(1, nt):
        pl.semaphore_signal(barrier, inc=1, device_id=dev(a, w, lax.rem(t + o, nt)), device_id_type=MESH)
    pl.semaphore_wait(barrier, na + nw + nt - 3)

    def a_copy(src, b, s, dr, h):
        return copy(src, abuf.at[b, h], a_send.at[dr, s, h], a_recv.at[dr, s + 1, h],
                    dev(a - (2 * dr - 1), w, t))

    for h in range(CHUNKS):
        for dr in range(2):
            target = a - (2 * dr - 1)

            @pl.when((target >= 0) & (target < na))
            def _():
                a_copy(hid.at[pl.ds(h * half, half), :], a, 0, dr, h).start()
    for o in range(1, nw):
        p = lax.rem(w + o, nw)
        copy(wei, wbuf.at[w], w_send.at[p], w_recv.at[w], dev(a, p, t)).start()
    locals_ = [pltpu.make_async_copy(wei, wbuf.at[w], loc_sem.at[CHUNKS])]
    locals_ += [
        pltpu.make_async_copy(hid.at[pl.ds(h * half, half), :], abuf.at[a, h], loc_sem.at[h])
        for h in range(CHUNKS)
    ]
    for c in locals_:
        c.start()
    for c in locals_:
        c.wait()

    def mm(b, h, slot):
        term = jnp.dot(abuf[b, h], wbuf[slot], preferred_element_type=jnp.float32)
        term = term.astype(pbuf.dtype)
        for k in range(nt):
            pbuf[b, h, k, slot] = term[k * rr:(k + 1) * rr]

    def p_copy(b, h, peer, me):
        return copy(pbuf.at[b, h, peer], rbuf.at[b, h, me], p_send.at[b, h, peer],
                    p_recv.at[b, h, me], dev(a, w, peer))

    def s_copy(b, h, src):
        return copy(sbuf.at[b, h], srec.at[src, h], s_send.at[b, h], s_recv.at[src, h], dev(b, w, t))

    def g_copy(src, h, peer, me):
        return copy(srec.at[src, h], gbuf.at[src, h, me], g_send.at[src, h, peer],
                    g_recv.at[src, h, me], dev(a, w, peer))

    def send_terms(b, h):
        for o in range(1, nt):
            p_copy(b, h, lax.rem(t + o, nt), t).start()

    def add_terms(b, h):
        total = pbuf[b, h, t].astype(jnp.float32)
        for o in range(1, nt):
            peer = lax.rem(t + o, nt)
            p_copy(b, h, peer, peer).wait_recv()
            total = total + rbuf[b, h, peer].astype(jnp.float32)
        total = total.astype(sbuf.dtype)

        @pl.when(b == a)
        def _():
            srec[b, h] = total

        @pl.when(b != a)
        def _():
            sbuf[b, h] = total
            s_copy(b, h, a).start()

    def spread(src, h):
        @pl.when(src != a)
        def _():
            s_copy(src, h, src).wait_recv()

        for o in range(1, nt):
            g_copy(src, h, lax.rem(t + o, nt), t).start()

    def loop(n, body):
        lax.fori_loop(0, n, lambda i, c: (body(i), c)[1], 0)

    loop(CHUNKS, lambda h: mm(a, h, w))

    def arrive(b, s, dr, h):
        a_copy(abuf.at[b, h], b, s - 1, dr, h).wait_recv()
        target = a - (2 * dr - 1)

        @pl.when((target >= 0) & (target < na))
        def _():
            a_copy(abuf.at[b, h], b, s, dr, h).start()

    def step(i):
        dr = lax.rem(i, 2)
        h = lax.rem(lax.div(i, 2), CHUNKS)
        s = lax.div(i, 2 * CHUNKS) + 1
        b = a + (2 * dr - 1) * s

        @pl.when((b >= 0) & (b < na))
        def _():
            arrive(b, s, dr, h)
            mm(b, h, w)

    loop((na - 2) * 2 * CHUNKS, step)

    for o in range(1, nw):
        p = lax.rem(w + o, nw)
        copy(wei, wbuf.at[p], w_send.at[p], w_recv.at[p], dev(a, p, t)).wait_recv()

    def near(i, body):
        b, h = lax.div(i, CHUNKS), lax.rem(i, CHUNKS)

        @pl.when((b - a <= na - 2) & (a - b <= na - 2))
        def _():
            body(b, h)

    def others(b, h):
        loop(nw - 1, lambda o: mm(b, h, lax.rem(w + 1 + o, nw)))
        send_terms(b, h)

    loop(na * CHUNKS, lambda i: near(i, others))
    loop(na * CHUNKS, lambda i: near(i, add_terms))
    loop(na * CHUNKS, lambda i: near(i, spread))

    @pl.when((a == 0) | (a == na - 1))
    def _():
        far = na - 1 - a
        dr = jnp.where(a == 0, 1, 0)

        def last(h):
            arrive(far, na - 1, dr, h)
            loop(nw, lambda o: mm(far, h, lax.rem(w + o, nw)))
            send_terms(far, h)
            add_terms(far, h)
            spread(far, h)

        loop(CHUNKS, last)

    def collect(i):
        b, h = lax.div(i, CHUNKS), lax.rem(i, CHUNKS)
        for o in range(1, nt):
            peer = lax.rem(t + o, nt)
            g_copy(b, h, peer, peer).wait_recv()
            out[b, h, peer] = gbuf[b, h, peer]
        out[b, h, t] = srec[b, h]

    loop(na * CHUNKS, collect)

    def drain(i):
        b, h = lax.div(i, CHUNKS), lax.rem(i, CHUNKS)
        for o in range(1, nt):
            peer = lax.rem(t + o, nt)
            p_copy(b, h, peer, t).wait_send()
            g_copy(b, h, peer, t).wait_send()

        @pl.when(b != a)
        def _():
            s_copy(b, h, a).wait_send()

    loop(na * CHUNKS, drain)

    def drain_a(i):
        dr = lax.rem(i, 2)
        h = lax.rem(lax.div(i, 2), CHUNKS)
        s = lax.div(i, 2 * CHUNKS)
        b = a + (2 * dr - 1) * s
        target = a - (2 * dr - 1)

        @pl.when((b >= 0) & (b < na) & (target >= 0) & (target < na))
        def _():
            a_copy(abuf.at[b, h], b, s, dr, h).wait_send()

    loop((na - 1) * 2 * CHUNKS, drain_a)
    for o in range(1, nw):
        p = lax.rem(w + o, nw)
        copy(wei, wbuf.at[w], w_send.at[p], w_recv.at[w], dev(a, p, t)).wait_send()


def peak_kernel(n, x, out, got, ss, rs):
    d = lax.axis_index("dp")
    t = lax.axis_index("tensor")
    barrier = pltpu.get_barrier_semaphore()
    for o in range(1, n):
        pl.semaphore_signal(barrier, inc=1, device_id=(lax.rem(d + o, n), t), device_id_type=MESH)
    pl.semaphore_wait(barrier, n - 1)

    def copy(o, slot):
        return pltpu.make_async_remote_copy(
            src_ref=x, dst_ref=got.at[slot], send_sem=ss.at[o], recv_sem=rs.at[slot],
            device_id=(lax.rem(d + o, n), t), device_id_type=MESH)

    for o in range(1, n):
        copy(o, o).start()
    best = x[...]
    for o in range(1, n):
        copy(o, o).wait_recv()
        best = jnp.maximum(best, got[o])
    for o in range(1, n):
        copy(o, o).wait_send()
    out[...] = best


def all_max(values, n):
    return pl.pallas_call(
        functools.partial(peak_kernel, n),
        out_shape=jax.ShapeDtypeStruct(values.shape, values.dtype),
        in_specs=[pl.BlockSpec(memory_space=pltpu.VMEM)],
        out_specs=pl.BlockSpec(memory_space=pltpu.VMEM),
        scratch_shapes=[
            pltpu.VMEM((n,) + values.shape, values.dtype),
            pltpu.SemaphoreType.DMA((n,)),
            pltpu.SemaphoreType.DMA((n,)),
        ],
        compiler_params=pltpu.CompilerParams(collective_id=1, has_side_effects=True),
    )(values)


def project(hidden, down_weight, long, short, nt):
    rows, depth = hidden.shape
    cols = down_weight.shape[1]
    na, nw = long[0], short[0]
    half = rows // CHUNKS
    rr = half // nt
    kind = hidden.dtype
    dma = pltpu.SemaphoreType.DMA
    return pl.pallas_call(
        functools.partial(project_kernel, (long, short, nt, half, rr)),
        out_shape=jax.ShapeDtypeStruct((na, CHUNKS, nt, nw, rr, cols), kind),
        in_specs=[pl.BlockSpec(memory_space=pl.ANY)] * 2,
        out_specs=pl.BlockSpec(memory_space=pltpu.VMEM),
        scratch_shapes=[
            pltpu.VMEM((na, CHUNKS, half, depth), kind),
            pltpu.VMEM((nw, depth, cols), kind),
            pltpu.VMEM((na, CHUNKS, nt, nw, rr, cols), kind),
            pltpu.VMEM((na, CHUNKS, nt, nw, rr, cols), kind),
            pltpu.VMEM((na, CHUNKS, nw, rr, cols), kind),
            pltpu.VMEM((na, CHUNKS, nw, rr, cols), kind),
            pltpu.VMEM((na, CHUNKS, nt, nw, rr, cols), kind),
            dma((CHUNKS + 1,)),
            dma((2, na, CHUNKS)), dma((2, na + 1, CHUNKS)),
            dma((nw,)), dma((nw,)),
            dma((na, CHUNKS, nt)), dma((na, CHUNKS, nt)),
            dma((na, CHUNKS)), dma((na, CHUNKS)),
            dma((na, CHUNKS, nt)), dma((na, CHUNKS, nt)),
        ],
        compiler_params=pltpu.CompilerParams(
            collective_id=0, has_side_effects=True, vmem_limit_bytes=60 * 1024 * 1024),
    )(hidden, down_weight)


def on_device(long, short, nt, hidden, down_weight, residual, post_gain, pre_gain, cast_scale, amax_history):
    stale_scale = cast_scale[0]
    parts = project(hidden, down_weight, long, short, nt)
    order = (1, 2, 4, 0, 3, 5) if long[1] > short[1] else (1, 2, 4, 3, 0, 5)
    summed = parts.transpose(order).reshape(residual.shape).astype(jnp.float32)
    stream = residual.astype(jnp.float32) + rms_norm(summed, post_gain)
    normed = rms_norm(stream, pre_gain)
    cast_out = (jnp.clip(normed * stale_scale, -float_limit, float_limit) / stale_scale).astype(
        jnp.bfloat16
    )
    peak_values = jnp.stack(
        [jnp.max(jnp.abs(summed)), jnp.max(jnp.abs(stream)), jnp.max(jnp.abs(normed))]
    )
    tile = jnp.zeros((8, 128), jnp.float32).at[:3, :].set(peak_values[:, None])
    peak_values = all_max(tile, long[0] * short[0])[:3, 0]
    new_history = jnp.concatenate([peak_values[:, None], amax_history[:, :-1]], axis=1)
    new_scales = float_limit / jnp.maximum(jnp.max(new_history, axis=1), 1.0)
    return (cast_out, stream.astype(jnp.bfloat16), peak_values, new_history, new_scales)


def solution(mesh):
    long, short = factor(mesh)
    in_specs = (P("dp", "tensor"), P("tensor", "dp"), P("dp", None), P(), P(), P(), P())
    out_specs = (P("dp", None), P("dp", None), P(), P(), P())
    return jax.shard_map(
        functools.partial(on_device, long, short, mesh.shape["tensor"]),
        mesh=mesh, in_specs=in_specs, out_specs=out_specs, check_vma=False
    )
```

```python
import functools

import jax
import jax.numpy as jnp
from jax import lax
from jax.experimental import pallas as pl
from jax.experimental.pallas import tpu as pltpu
from jax.sharding import PartitionSpec as P

MESH = pl.DeviceIdType.MESH
norm_epsilon = 1e-06
float_limit = 448.0
CHUNKS = 2


def rms_norm(values, gain_vector):
    return (
        values
        * lax.rsqrt(jnp.mean(values * values, axis=-1, keepdims=True) + norm_epsilon)
        * gain_vector
    )


def factor(mesh):
    devices = mesh.devices
    count = devices.shape[0]
    coords = [tuple(devices[i, 0].coords) for i in range(count)]
    inner = 1
    if count > 1:
        axis = [p != q for p, q in zip(coords[0], coords[1])].index(True)
        while inner < count and all(
            p == q for k, (p, q) in enumerate(zip(coords[0], coords[inner])) if k != axis
        ):
            inner += 1
    outer = count // inner
    if outer >= inner:
        return (outer, inner), (inner, 1)
    return (inner, 1), (outer, inner)


def project_kernel(dims, hid, wei, out, abuf, wbuf, pbuf, rbuf, sbuf, srec, gbuf,
                   loc_sem, a_send, a_recv, w_send, w_recv, p_send, p_recv,
                   s_send, s_recv, g_send, g_recv):
    (na, sa), (nw, sw), nt, half, rr = dims
    d = lax.axis_index("dp")
    t = lax.axis_index("tensor")
    a = lax.rem(lax.div(d, sa), na)
    w = lax.rem(lax.div(d, sw), nw)

    def dev(a_, w_, t_):
        return (a_ * sa + w_ * sw, t_)

    def copy(src, dst, ss, rs, to):
        return pltpu.make_async_remote_copy(
            src_ref=src, dst_ref=dst, send_sem=ss, recv_sem=rs,
            device_id=to, device_id_type=MESH)

    barrier = pltpu.get_barrier_semaphore()
    for o in range(1, na):
        pl.semaphore_signal(barrier, inc=1, device_id=dev(lax.rem(a + o, na), w, t), device_id_type=MESH)
    for o in range(1, nw):
        pl.semaphore_signal(barrier, inc=1, device_id=dev(a, lax.rem(w + o, nw), t), device_id_type=MESH)
    for o in range(1, nt):
        pl.semaphore_signal(barrier, inc=1, device_id=dev(a, w, lax.rem(t + o, nt)), device_id_type=MESH)
    pl.semaphore_wait(barrier, na + nw + nt - 3)

    def a_copy(src, b, s, dr, h):
        return copy(src, abuf.at[b, h], a_send.at[dr, s, h], a_recv.at[dr, s + 1, h],
                    dev(a - (2 * dr - 1), w, t))

    for h in range(CHUNKS):
        for dr in range(2):
            target = a - (2 * dr - 1)

            @pl.when((target >= 0) & (target < na))
            def _():
                a_copy(hid.at[pl.ds(h * half, half), :], a, 0, dr, h).start()
    for o in range(1, nw):
        p = lax.rem(w + o, nw)
        copy(wei, wbuf.at[w], w_send.at[p], w_recv.at[w], dev(a, p, t)).start()
    locals_ = [pltpu.make_async_copy(wei, wbuf.at[w], loc_sem.at[CHUNKS])]
    locals_ += [
        pltpu.make_async_copy(hid.at[pl.ds(h * half, half), :], abuf.at[a, h], loc_sem.at[h])
        for h in range(CHUNKS)
    ]
    for c in locals_:
        c.start()
    for c in locals_:
        c.wait()

    def mm(b, h, slot):
        term = lax.dot_general(
            abuf[b, h], wbuf[slot], (((1,), (1,)), ((), ())),
            preferred_element_type=jnp.float32)
        term = term.astype(pbuf.dtype)
        for k in range(nt):
            pbuf[b, h, k, slot] = term[k * rr:(k + 1) * rr]

    def p_copy(b, h, slot, peer, me):
        return copy(pbuf.at[b, h, peer, slot], rbuf.at[b, h, me, slot],
                    p_send.at[b, h, peer, slot], p_recv.at[b, h, me, slot], dev(a, w, peer))

    def s_copy(b, h, slot, src):
        return copy(sbuf.at[b, h, slot], srec.at[src, h, slot], s_send.at[b, h, slot],
                    s_recv.at[src, h, slot], dev(b, w, t))

    def g_copy(src, h, slot, peer, me):
        return copy(srec.at[src, h, slot], gbuf.at[src, h, me, slot],
                    g_send.at[src, h, peer, slot], g_recv.at[src, h, me, slot], dev(a, w, peer))

    def send_terms(b, h, slot):
        for o in range(1, nt):
            p_copy(b, h, slot, lax.rem(t + o, nt), t).start()

    def add_terms(b, h, slot):
        total = pbuf[b, h, t, slot].astype(jnp.float32)
        for o in range(1, nt):
            peer = lax.rem(t + o, nt)
            p_copy(b, h, slot, peer, peer).wait_recv()
            total = total + rbuf[b, h, peer, slot].astype(jnp.float32)
        total = total.astype(sbuf.dtype)

        @pl.when(b == a)
        def _():
            srec[b, h, slot] = total

        @pl.when(b != a)
        def _():
            sbuf[b, h, slot] = total
            s_copy(b, h, slot, a).start()

    def spread(src, h, slot):
        @pl.when(src != a)
        def _():
            s_copy(src, h, slot, src).wait_recv()

        for o in range(1, nt):
            g_copy(src, h, slot, lax.rem(t + o, nt), t).start()

    def loop(n, body):
        lax.fori_loop(0, n, lambda i, c: (body(i), c)[1], 0)

    def own(h):
        mm(a, h, w)
        send_terms(a, h, w)

    loop(CHUNKS, own)

    def arrive(b, s, dr, h):
        a_copy(abuf.at[b, h], b, s - 1, dr, h).wait_recv()
        target = a - (2 * dr - 1)

        @pl.when((target >= 0) & (target < na))
        def _():
            a_copy(abuf.at[b, h], b, s, dr, h).start()

    def step(i):
        dr = lax.rem(i, 2)
        h = lax.rem(lax.div(i, 2), CHUNKS)
        s = lax.div(i, 2 * CHUNKS) + 1
        b = a + (2 * dr - 1) * s

        @pl.when((b >= 0) & (b < na))
        def _():
            arrive(b, s, dr, h)
            mm(b, h, w)
            send_terms(b, h, w)

    loop((na - 2) * 2 * CHUNKS, step)

    def near(i, body):
        b, h = lax.div(i, CHUNKS), lax.rem(i, CHUNKS)

        @pl.when((b - a <= na - 2) & (a - b <= na - 2))
        def _():
            body(b, h)

    loop(na * CHUNKS, lambda i: near(i, lambda b, h: add_terms(b, h, w)))
    loop(na * CHUNKS, lambda i: near(i, lambda b, h: spread(b, h, w)))

    for o in range(1, nw):
        p = lax.rem(w + o, nw)
        copy(wei, wbuf.at[p], w_send.at[p], w_recv.at[p], dev(a, p, t)).wait_recv()

    def each_other(body):
        return lambda b, h: loop(nw - 1, lambda o: body(b, h, lax.rem(w + 1 + o, nw)))

    def multiply(b, h, slot):
        mm(b, h, slot)
        send_terms(b, h, slot)

    loop(na * CHUNKS, lambda i: near(i, each_other(multiply)))
    loop(na * CHUNKS, lambda i: near(i, each_other(add_terms)))
    loop(na * CHUNKS, lambda i: near(i, each_other(spread)))

    @pl.when((a == 0) | (a == na - 1))
    def _():
        far = na - 1 - a
        dr = jnp.where(a == 0, 1, 0)

        def last(h):
            arrive(far, na - 1, dr, h)
            loop(nw, lambda slot: multiply(far, h, slot))
            loop(nw, lambda slot: add_terms(far, h, slot))
            loop(nw, lambda slot: spread(far, h, slot))

        loop(CHUNKS, last)

    def collect(i):
        b, h = lax.div(i, CHUNKS), lax.rem(i, CHUNKS)
        for o in range(1, nt):
            peer = lax.rem(t + o, nt)
            for slot in range(nw):
                g_copy(b, h, slot, peer, peer).wait_recv()
            out[b, h, peer] = gbuf[b, h, peer]
        out[b, h, t] = srec[b, h]

    loop(na * CHUNKS, collect)

    def drain(i):
        b, h = lax.div(i, CHUNKS), lax.rem(i, CHUNKS)
        for slot in range(nw):
            for o in range(1, nt):
                peer = lax.rem(t + o, nt)
                p_copy(b, h, slot, peer, t).wait_send()
                g_copy(b, h, slot, peer, t).wait_send()

            @pl.when(b != a)
            def _():
                s_copy(b, h, slot, a).wait_send()

    loop(na * CHUNKS, drain)

    def drain_a(i):
        dr = lax.rem(i, 2)
        h = lax.rem(lax.div(i, 2), CHUNKS)
        s = lax.div(i, 2 * CHUNKS)
        b = a + (2 * dr - 1) * s
        target = a - (2 * dr - 1)

        @pl.when((b >= 0) & (b < na) & (target >= 0) & (target < na))
        def _():
            a_copy(abuf.at[b, h], b, s, dr, h).wait_send()

    loop((na - 1) * 2 * CHUNKS, drain_a)
    for o in range(1, nw):
        p = lax.rem(w + o, nw)
        copy(wei, wbuf.at[w], w_send.at[p], w_recv.at[w], dev(a, p, t)).wait_send()


def peak_kernel(n, x, hist, peaks, history, scales, got, ss, rs):
    d = lax.axis_index("dp")
    t = lax.axis_index("tensor")
    barrier = pltpu.get_barrier_semaphore()
    for o in range(1, n):
        pl.semaphore_signal(barrier, inc=1, device_id=(lax.rem(d + o, n), t), device_id_type=MESH)
    pl.semaphore_wait(barrier, n - 1)

    def copy(o, slot):
        return pltpu.make_async_remote_copy(
            src_ref=x, dst_ref=got.at[slot], send_sem=ss.at[o], recv_sem=rs.at[slot],
            device_id=(lax.rem(d + o, n), t), device_id_type=MESH)

    for o in range(1, n):
        copy(o, o).start()
    best = x[...]
    for o in range(1, n):
        copy(o, o).wait_recv()
        best = jnp.maximum(best, got[o])
    best = best[:3, :1]
    kept = hist[...]
    lane = lax.broadcasted_iota(jnp.int32, kept.shape, 1)
    new = jnp.where(lane == 0, best, pltpu.roll(kept, 1, 1))
    peaks[...] = best
    history[...] = new
    scales[...] = float_limit / jnp.maximum(jnp.max(new, axis=1, keepdims=True), 1.0)
    for o in range(1, n):
        copy(o, o).wait_send()


def all_max(values, hist, n):
    vmem = pl.BlockSpec(memory_space=pltpu.VMEM)
    column = jax.ShapeDtypeStruct((hist.shape[0], 1), jnp.float32)
    return pl.pallas_call(
        functools.partial(peak_kernel, n),
        out_shape=(column, jax.ShapeDtypeStruct(hist.shape, hist.dtype), column),
        in_specs=[vmem] * 2,
        out_specs=[vmem] * 3,
        scratch_shapes=[
            pltpu.VMEM((n,) + values.shape, values.dtype),
            pltpu.SemaphoreType.DMA((n,)),
            pltpu.SemaphoreType.DMA((n,)),
        ],
        compiler_params=pltpu.CompilerParams(collective_id=1, has_side_effects=True),
    )(values, hist)


def finish_kernel(dims, scale, parts, residual, post_gain, pre_gain, cast_out, stream_out, peaks, summed):
    (na, sa), (nw, sw), cols = dims
    for a in range(na):
        for w in range(nw):
            first = (a * sa + w * sw) * cols
            summed[:, first:first + cols] = parts[a, 0, 0, w].astype(jnp.float32)
    x = summed[...]
    stream = residual[...].astype(jnp.float32) + rms_norm(x, post_gain[...])
    normed = rms_norm(stream, pre_gain[...])
    s = scale[0]
    cast_out[...] = (jnp.clip(normed * s, -float_limit, float_limit) / s).astype(cast_out.dtype)
    stream_out[...] = stream.astype(stream_out.dtype)
    row = lax.broadcasted_iota(jnp.int32, peaks.shape, 0)
    tops = [jnp.max(jnp.abs(v)) for v in (x, stream, normed)]
    tile = jnp.where(row == 0, tops[0], jnp.where(row == 1, tops[1], tops[2]))
    first_step = (pl.program_id(0) == 0) & (pl.program_id(1) == 0)

    @pl.when(first_step)
    def _():
        peaks[...] = tile

    @pl.when(jnp.logical_not(first_step))
    def _():
        peaks[...] = jnp.maximum(peaks[...], tile)


def finish(parts, residual, post_gain, pre_gain, cast_scale, long, short):
    na, chunks, nt, nw, rr, cols = parts.shape
    width = residual.shape[1]
    rows = pl.BlockSpec((rr, width), lambda h, k: (h * nt + k, 0))
    gain = pl.BlockSpec((1, width), lambda h, k: (0, 0))
    kind = jax.ShapeDtypeStruct(residual.shape, jnp.bfloat16)
    return pl.pallas_call(
        functools.partial(finish_kernel, (long, short, cols)),
        grid=(chunks, nt),
        out_shape=(kind, kind, jax.ShapeDtypeStruct((8, 128), jnp.float32)),
        in_specs=[
            pl.BlockSpec(memory_space=pltpu.SMEM),
            pl.BlockSpec((na, 1, 1, nw, rr, cols), lambda h, k: (0, h, k, 0, 0, 0)),
            rows, gain, gain,
        ],
        out_specs=[rows, rows, pl.BlockSpec((8, 128), lambda h, k: (0, 0))],
        scratch_shapes=[pltpu.VMEM((rr, width), jnp.float32)],
    )(cast_scale, parts, residual, post_gain[None], pre_gain[None])


def project(hidden, down_weight, long, short, nt):
    rows, depth = hidden.shape
    cols = down_weight.shape[0]
    na, nw = long[0], short[0]
    half = rows // CHUNKS
    rr = half // nt
    kind = hidden.dtype
    dma = pltpu.SemaphoreType.DMA
    return pl.pallas_call(
        functools.partial(project_kernel, (long, short, nt, half, rr)),
        out_shape=jax.ShapeDtypeStruct((na, CHUNKS, nt, nw, rr, cols), kind),
        in_specs=[pl.BlockSpec(memory_space=pl.ANY)] * 2,
        out_specs=pl.BlockSpec(memory_space=pltpu.VMEM),
        scratch_shapes=[
            pltpu.VMEM((na, CHUNKS, half, depth), kind),
            pltpu.VMEM((nw, cols, depth), kind),
            pltpu.VMEM((na, CHUNKS, nt, nw, rr, cols), kind),
            pltpu.VMEM((na, CHUNKS, nt, nw, rr, cols), kind),
            pltpu.VMEM((na, CHUNKS, nw, rr, cols), kind),
            pltpu.VMEM((na, CHUNKS, nw, rr, cols), kind),
            pltpu.VMEM((na, CHUNKS, nt, nw, rr, cols), kind),
            dma((CHUNKS + 1,)),
            dma((2, na, CHUNKS)), dma((2, na + 1, CHUNKS)),
            dma((nw,)), dma((nw,)),
            dma((na, CHUNKS, nt, nw)), dma((na, CHUNKS, nt, nw)),
            dma((na, CHUNKS, nw)), dma((na, CHUNKS, nw)),
            dma((na, CHUNKS, nt, nw)), dma((na, CHUNKS, nt, nw)),
        ],
        compiler_params=pltpu.CompilerParams(
            collective_id=0, has_side_effects=True, vmem_limit_bytes=60 * 1024 * 1024),
    )(hidden, down_weight)


def on_device(long, short, nt, hidden, down_weight, residual, post_gain, pre_gain, cast_scale, amax_history):
    parts = project(hidden, down_weight.T, long, short, nt)
    cast_out, stream, tile = finish(parts, residual, post_gain, pre_gain, cast_scale, long, short)
    peaks, new_history, new_scales = all_max(tile, amax_history, long[0] * short[0])
    return (cast_out, stream, peaks[:, 0], new_history, new_scales[:, 0])


def solution(mesh):
    long, short = factor(mesh)
    in_specs = (P("dp", "tensor"), P("tensor", "dp"), P("dp", None), P(), P(), P(), P())
    out_specs = (P("dp", None), P("dp", None), P(), P(), P())
    return jax.shard_map(
        functools.partial(on_device, long, short, mesh.shape["tensor"]),
        mesh=mesh, in_specs=in_specs, out_specs=out_specs, check_vma=False
    )
```

```python
import functools

import jax
import jax.numpy as jnp
from jax import lax
from jax.experimental import pallas as pl
from jax.experimental.pallas import tpu as pltpu
from jax.sharding import PartitionSpec as P

MESH = pl.DeviceIdType.MESH
norm_epsilon = 1e-06
float_limit = 448.0
CHUNKS = 2


def rms_norm(values, gain_vector):
    return (
        values
        * lax.rsqrt(jnp.mean(values * values, axis=-1, keepdims=True) + norm_epsilon)
        * gain_vector
    )


def factor(mesh):
    devices = mesh.devices
    count = devices.shape[0]
    coords = [tuple(devices[i, 0].coords) for i in range(count)]
    inner = 1
    if count > 1:
        axis = [p != q for p, q in zip(coords[0], coords[1])].index(True)
        while inner < count and all(
            p == q for k, (p, q) in enumerate(zip(coords[0], coords[inner])) if k != axis
        ):
            inner += 1
    outer = count // inner
    if outer >= inner:
        return (outer, inner), (inner, 1)
    return (inner, 1), (outer, inner)


def project_kernel(dims, hid, wei, out, abuf, wbuf, pbuf, rbuf, sbuf, srec, gbuf,
                   loc_sem, a_send, a_recv, w_send, w_recv, p_send, p_recv,
                   s_send, s_recv, g_send, g_recv):
    (na, sa), (nw, sw), nt, half, rr = dims
    d = lax.axis_index("dp")
    t = lax.axis_index("tensor")
    a = lax.rem(lax.div(d, sa), na)
    w = lax.rem(lax.div(d, sw), nw)

    def dev(a_, w_, t_):
        return (a_ * sa + w_ * sw, t_)

    def copy(src, dst, ss, rs, to):
        return pltpu.make_async_remote_copy(
            src_ref=src, dst_ref=dst, send_sem=ss, recv_sem=rs,
            device_id=to, device_id_type=MESH)

    barrier = pltpu.get_barrier_semaphore()
    for o in range(1, na):
        pl.semaphore_signal(barrier, inc=1, device_id=dev(lax.rem(a + o, na), w, t), device_id_type=MESH)
    for o in range(1, nw):
        pl.semaphore_signal(barrier, inc=1, device_id=dev(a, lax.rem(w + o, nw), t), device_id_type=MESH)
    for o in range(1, nt):
        pl.semaphore_signal(barrier, inc=1, device_id=dev(a, w, lax.rem(t + o, nt)), device_id_type=MESH)
    pl.semaphore_wait(barrier, na + nw + nt - 3)

    def a_copy(src, b, s, dr, h):
        return copy(src, abuf.at[b, h], a_send.at[dr, s, h], a_recv.at[dr, s + 1, h],
                    dev(a - (2 * dr - 1), w, t))

    for h in range(CHUNKS):
        for dr in range(2):
            target = a - (2 * dr - 1)

            @pl.when((target >= 0) & (target < na))
            def _():
                a_copy(hid.at[pl.ds(h * half, half), :], a, 0, dr, h).start()
    for o in range(1, nw):
        p = lax.rem(w + o, nw)
        copy(wei, wbuf.at[w], w_send.at[p], w_recv.at[w], dev(a, p, t)).start()
    locals_ = [pltpu.make_async_copy(wei, wbuf.at[w], loc_sem.at[CHUNKS])]
    locals_ += [
        pltpu.make_async_copy(hid.at[pl.ds(h * half, half), :], abuf.at[a, h], loc_sem.at[h])
        for h in range(CHUNKS)
    ]
    for c in locals_:
        c.start()
    for c in locals_:
        c.wait()

    def mm(b, h, slot):
        term = lax.dot_general(
            abuf[b, h], wbuf[slot], (((1,), (1,)), ((), ())),
            preferred_element_type=jnp.float32)
        term = term.astype(pbuf.dtype)
        for k in range(nt):
            pbuf[b, h, k, slot] = term[k * rr:(k + 1) * rr]

    def mm_whole(b, slot):
        rows = abuf[b].reshape(CHUNKS * half, abuf.shape[-1])
        term = lax.dot_general(
            rows, wbuf[slot], (((1,), (1,)), ((), ())), preferred_element_type=jnp.float32)
        term = term.astype(pbuf.dtype)
        for h in range(CHUNKS):
            for k in range(nt):
                first = h * half + k * rr
                pbuf[b, h, k, slot] = term[first:first + rr]

    def p_copy(b, h, slot, peer, me):
        return copy(pbuf.at[b, h, peer, slot], rbuf.at[b, h, me, slot],
                    p_send.at[b, h, peer, slot], p_recv.at[b, h, me, slot], dev(a, w, peer))

    def s_copy(b, h, slot, src):
        return copy(sbuf.at[b, h, slot], srec.at[src, h, slot], s_send.at[b, h, slot],
                    s_recv.at[src, h, slot], dev(b, w, t))

    def g_copy(src, h, slot, peer, me):
        return copy(srec.at[src, h, slot], gbuf.at[src, h, me, slot],
                    g_send.at[src, h, peer, slot], g_recv.at[src, h, me, slot], dev(a, w, peer))

    def send_terms(b, h, slot):
        for o in range(1, nt):
            p_copy(b, h, slot, lax.rem(t + o, nt), t).start()

    def add_terms(b, h, slot):
        total = pbuf[b, h, t, slot].astype(jnp.float32)
        for o in range(1, nt):
            peer = lax.rem(t + o, nt)
            p_copy(b, h, slot, peer, peer).wait_recv()
            total = total + rbuf[b, h, peer, slot].astype(jnp.float32)
        total = total.astype(sbuf.dtype)

        @pl.when(b == a)
        def _():
            srec[b, h, slot] = total

        @pl.when(b != a)
        def _():
            sbuf[b, h, slot] = total
            s_copy(b, h, slot, a).start()

    def spread(src, h, slot):
        @pl.when(src != a)
        def _():
            s_copy(src, h, slot, src).wait_recv()

        for o in range(1, nt):
            g_copy(src, h, slot, lax.rem(t + o, nt), t).start()

    def loop(n, body):
        lax.fori_loop(0, n, lambda i, c: (body(i), c)[1], 0)

    def own(h):
        mm(a, h, w)
        send_terms(a, h, w)
        add_terms(a, h, w)

    loop(CHUNKS, own)

    def arrive(b, s, dr, h):
        a_copy(abuf.at[b, h], b, s - 1, dr, h).wait_recv()
        target = a - (2 * dr - 1)

        @pl.when((target >= 0) & (target < na))
        def _():
            a_copy(abuf.at[b, h], b, s, dr, h).start()

    def step(i):
        dr = lax.rem(i, 2)
        h = lax.rem(lax.div(i, 2), CHUNKS)
        s = lax.div(i, 2 * CHUNKS) + 1
        b = a + (2 * dr - 1) * s

        @pl.when((b >= 0) & (b < na))
        def _():
            arrive(b, s, dr, h)
            mm(b, h, w)
            send_terms(b, h, w)
            add_terms(b, h, w)

    loop((na - 2) * 2 * CHUNKS, step)

    def near(i, body):
        b, h = lax.div(i, CHUNKS), lax.rem(i, CHUNKS)

        @pl.when((b - a <= na - 2) & (a - b <= na - 2))
        def _():
            body(b, h)


    for o in range(1, nw):
        p = lax.rem(w + o, nw)
        copy(wei, wbuf.at[p], w_send.at[p], w_recv.at[p], dev(a, p, t)).wait_recv()

    def each_other(body):
        return lambda b, h: loop(nw - 1, lambda o: body(b, h, lax.rem(w + 1 + o, nw)))

    def multiply(b, h, slot):
        mm(b, h, slot)
        send_terms(b, h, slot)

    def multiply_whole(b):
        @pl.when((b - a <= na - 2) & (a - b <= na - 2))
        def _():
            def one(o):
                slot = lax.rem(w + 1 + o, nw)
                mm_whole(b, slot)
                loop(CHUNKS, lambda h: send_terms(b, h, slot))

            loop(nw - 1, one)

    def late(h):
        far = na - 1 - a
        arrive(far, na - 1, jnp.where(a == 0, 1, 0), h)
        loop(nw, lambda slot: multiply(far, h, slot))
        loop(nw, lambda slot: add_terms(far, h, slot))

    end = (a == 0) | (a == na - 1)
    loop(na, multiply_whole)
    loop(na * CHUNKS, lambda i: near(i, each_other(add_terms)))
    loop(na * CHUNKS, lambda i: near(i, lambda b, h: spread(b, h, w)))
    pl.when(end)(lambda: loop(CHUNKS - 1, late))

    def prompt(b, h):
        pl.when((b - a != 1) & (a - b != 1))(lambda: each_other(spread)(b, h))

    def queued(b, h):
        pl.when((b - a == 1) | (a - b == 1))(lambda: each_other(spread)(b, h))

    loop(na * CHUNKS, lambda i: near(i, prompt))
    pl.when(end)(lambda: late(CHUNKS - 1))
    loop(na * CHUNKS, lambda i: near(i, queued))

    @pl.when(end)
    def _():
        loop(CHUNKS, lambda h: loop(nw, lambda slot: spread(na - 1 - a, h, slot)))

    def collect(i):
        b, h = lax.div(i, CHUNKS), lax.rem(i, CHUNKS)
        for o in range(1, nt):
            peer = lax.rem(t + o, nt)
            for slot in range(nw):
                g_copy(b, h, slot, peer, peer).wait_recv()
            out[b, h, peer] = gbuf[b, h, peer]
        out[b, h, t] = srec[b, h]

    loop(na * CHUNKS, collect)

    def drain(i):
        b, h = lax.div(i, CHUNKS), lax.rem(i, CHUNKS)
        for slot in range(nw):
            for o in range(1, nt):
                peer = lax.rem(t + o, nt)
                p_copy(b, h, slot, peer, t).wait_send()
                g_copy(b, h, slot, peer, t).wait_send()

            @pl.when(b != a)
            def _():
                s_copy(b, h, slot, a).wait_send()

    loop(na * CHUNKS, drain)

    def drain_a(i):
        dr = lax.rem(i, 2)
        h = lax.rem(lax.div(i, 2), CHUNKS)
        s = lax.div(i, 2 * CHUNKS)
        b = a + (2 * dr - 1) * s
        target = a - (2 * dr - 1)

        @pl.when((b >= 0) & (b < na) & (target >= 0) & (target < na))
        def _():
            a_copy(abuf.at[b, h], b, s, dr, h).wait_send()

    loop((na - 1) * 2 * CHUNKS, drain_a)
    for o in range(1, nw):
        p = lax.rem(w + o, nw)
        copy(wei, wbuf.at[w], w_send.at[p], w_recv.at[w], dev(a, p, t)).wait_send()


def peak_kernel(n, x, hist, peaks, history, scales, got, ss, rs):
    d = lax.axis_index("dp")
    t = lax.axis_index("tensor")
    barrier = pltpu.get_barrier_semaphore()
    for o in range(1, n):
        pl.semaphore_signal(barrier, inc=1, device_id=(lax.rem(d + o, n), t), device_id_type=MESH)
    pl.semaphore_wait(barrier, n - 1)

    def copy(o, slot):
        return pltpu.make_async_remote_copy(
            src_ref=x, dst_ref=got.at[slot], send_sem=ss.at[o], recv_sem=rs.at[slot],
            device_id=(lax.rem(d + o, n), t), device_id_type=MESH)

    for o in range(1, n):
        copy(o, o).start()
    best = x[...]
    for o in range(1, n):
        copy(o, o).wait_recv()
        best = jnp.maximum(best, got[o])
    best = best[:3, :1]
    kept = hist[...]
    lane = lax.broadcasted_iota(jnp.int32, kept.shape, 1)
    new = jnp.where(lane == 0, best, pltpu.roll(kept, 1, 1))
    history[...] = new
    scale = float_limit / jnp.maximum(jnp.max(new, axis=1, keepdims=True), 1.0)
    for i in range(kept.shape[0]):
        peaks[i] = best[i, 0]
        scales[i] = scale[i, 0]
    for o in range(1, n):
        copy(o, o).wait_send()


def all_max(values, hist, n):
    vmem = pl.BlockSpec(memory_space=pltpu.VMEM)
    column = jax.ShapeDtypeStruct((hist.shape[0],), jnp.float32)
    smem = pl.BlockSpec(memory_space=pltpu.SMEM)
    return pl.pallas_call(
        functools.partial(peak_kernel, n),
        out_shape=(column, jax.ShapeDtypeStruct(hist.shape, hist.dtype), column),
        in_specs=[vmem] * 2,
        out_specs=[smem, vmem, smem],
        scratch_shapes=[
            pltpu.VMEM((n,) + values.shape, values.dtype),
            pltpu.SemaphoreType.DMA((n,)),
            pltpu.SemaphoreType.DMA((n,)),
        ],
        compiler_params=pltpu.CompilerParams(collective_id=1, has_side_effects=True),
    )(values, hist)


def finish_kernel(dims, scale, parts, residual, post_gain, pre_gain, cast_out, stream_out, peaks, summed):
    (na, sa), (nw, sw), cols = dims
    for a in range(na):
        for w in range(nw):
            first = (a * sa + w * sw) * cols
            summed[:, first:first + cols] = parts[a, 0, 0, w].astype(jnp.float32)
    x = summed[...]
    stream = residual[...].astype(jnp.float32) + rms_norm(x, post_gain[...].reshape(1, -1))
    normed = rms_norm(stream, pre_gain[...].reshape(1, -1))
    s = scale[0]
    cast_out[...] = (jnp.clip(normed * s, -float_limit, float_limit) / s).astype(cast_out.dtype)
    stream_out[...] = stream.astype(stream_out.dtype)
    row = lax.broadcasted_iota(jnp.int32, peaks.shape, 0)
    tops = [jnp.max(jnp.abs(v)) for v in (x, stream, normed)]
    tile = jnp.where(row == 0, tops[0], jnp.where(row == 1, tops[1], tops[2]))
    first_step = (pl.program_id(0) == 0) & (pl.program_id(1) == 0)

    @pl.when(first_step)
    def _():
        peaks[...] = tile

    @pl.when(jnp.logical_not(first_step))
    def _():
        peaks[...] = jnp.maximum(peaks[...], tile)


def finish(parts, residual, post_gain, pre_gain, cast_scale, long, short):
    na, chunks, nt, nw, rr, cols = parts.shape
    width = residual.shape[1]
    rows = pl.BlockSpec((rr, width), lambda h, k: (h * nt + k, 0))
    gain = pl.BlockSpec((width,), lambda h, k: (0,))
    kind = jax.ShapeDtypeStruct(residual.shape, jnp.bfloat16)
    return pl.pallas_call(
        functools.partial(finish_kernel, (long, short, cols)),
        grid=(chunks, nt),
        out_shape=(kind, kind, jax.ShapeDtypeStruct((8, 128), jnp.float32)),
        in_specs=[
            pl.BlockSpec(memory_space=pltpu.SMEM),
            pl.BlockSpec((na, 1, 1, nw, rr, cols), lambda h, k: (0, h, k, 0, 0, 0)),
            rows, gain, gain,
        ],
        out_specs=[rows, rows, pl.BlockSpec((8, 128), lambda h, k: (0, 0))],
        scratch_shapes=[pltpu.VMEM((rr, width), jnp.float32)],
    )(cast_scale, parts, residual, post_gain, pre_gain)


def project(hidden, down_weight, long, short, nt):
    rows, depth = hidden.shape
    cols = down_weight.shape[0]
    na, nw = long[0], short[0]
    half = rows // CHUNKS
    rr = half // nt
    kind = hidden.dtype
    dma = pltpu.SemaphoreType.DMA
    return pl.pallas_call(
        functools.partial(project_kernel, (long, short, nt, half, rr)),
        out_shape=jax.ShapeDtypeStruct((na, CHUNKS, nt, nw, rr, cols), kind),
        in_specs=[pl.BlockSpec(memory_space=pl.ANY)] * 2,
        out_specs=pl.BlockSpec(memory_space=pltpu.VMEM),
        scratch_shapes=[
            pltpu.VMEM((na, CHUNKS, half, depth), kind),
            pltpu.VMEM((nw, cols, depth), kind),
            pltpu.VMEM((na, CHUNKS, nt, nw, rr, cols), kind),
            pltpu.VMEM((na, CHUNKS, nt, nw, rr, cols), kind),
            pltpu.VMEM((na, CHUNKS, nw, rr, cols), kind),
            pltpu.VMEM((na, CHUNKS, nw, rr, cols), kind),
            pltpu.VMEM((na, CHUNKS, nt, nw, rr, cols), kind),
            dma((CHUNKS + 1,)),
            dma((2, na, CHUNKS)), dma((2, na + 1, CHUNKS)),
            dma((nw,)), dma((nw,)),
            dma((na, CHUNKS, nt, nw)), dma((na, CHUNKS, nt, nw)),
            dma((na, CHUNKS, nw)), dma((na, CHUNKS, nw)),
            dma((na, CHUNKS, nt, nw)), dma((na, CHUNKS, nt, nw)),
        ],
        compiler_params=pltpu.CompilerParams(
            collective_id=0, has_side_effects=True, vmem_limit_bytes=60 * 1024 * 1024),
    )(hidden, down_weight)


def on_device(long, short, nt, hidden, down_weight, residual, post_gain, pre_gain, cast_scale, amax_history):
    parts = project(hidden, down_weight.T, long, short, nt)
    cast_out, stream, tile = finish(parts, residual, post_gain, pre_gain, cast_scale, long, short)
    peaks, new_history, new_scales = all_max(tile, amax_history, long[0] * short[0])
    return (cast_out, stream, peaks, new_history, new_scales)


def solution(mesh):
    long, short = factor(mesh)
    in_specs = (P("dp", "tensor"), P("tensor", "dp"), P("dp", None), P(), P(), P(), P())
    out_specs = (P("dp", None), P("dp", None), P(), P(), P())
    return jax.shard_map(
        functools.partial(on_device, long, short, mesh.shape["tensor"]),
        mesh=mesh, in_specs=in_specs, out_specs=out_specs, check_vma=False
    )
```

```python
import functools

import jax
import jax.numpy as jnp
from jax import lax
from jax.experimental import pallas as pl
from jax.experimental.pallas import tpu as pltpu
from jax.sharding import PartitionSpec as P

MESH = pl.DeviceIdType.MESH
norm_epsilon = 1e-06
float_limit = 448.0
CHUNKS = 2


def rms_norm(values, gain_vector):
    return (
        values
        * lax.rsqrt(jnp.mean(values * values, axis=-1, keepdims=True) + norm_epsilon)
        * gain_vector
    )


def factor(mesh):
    devices = mesh.devices
    count = devices.shape[0]
    coords = [tuple(devices[i, 0].coords) for i in range(count)]
    inner = 1
    if count > 1:
        axis = [p != q for p, q in zip(coords[0], coords[1])].index(True)
        while inner < count and all(
            p == q for k, (p, q) in enumerate(zip(coords[0], coords[inner])) if k != axis
        ):
            inner += 1
    outer = count // inner
    if outer >= inner:
        return (outer, inner), (inner, 1)
    return (inner, 1), (outer, inner)


def project_kernel(dims, hid, wei, out, abuf, wbuf, pbuf, rbuf, sbuf, srec, gbuf,
                   loc_sem, a_send, a_recv, w_send, w_recv, p_send, p_recv,
                   s_send, s_recv, g_send, g_recv):
    (na, sa), (nw, sw), nt, half, rr = dims
    d = lax.axis_index("dp")
    t = lax.axis_index("tensor")
    a = lax.rem(lax.div(d, sa), na)
    w = lax.rem(lax.div(d, sw), nw)

    def dev(a_, w_, t_):
        return (a_ * sa + w_ * sw, t_)

    def copy(src, dst, ss, rs, to):
        return pltpu.make_async_remote_copy(
            src_ref=src, dst_ref=dst, send_sem=ss, recv_sem=rs,
            device_id=to, device_id_type=MESH)

    barrier = pltpu.get_barrier_semaphore()
    for o in range(1, na):
        pl.semaphore_signal(barrier, inc=1, device_id=dev(lax.rem(a + o, na), w, t), device_id_type=MESH)
    for o in range(1, nw):
        pl.semaphore_signal(barrier, inc=1, device_id=dev(a, lax.rem(w + o, nw), t), device_id_type=MESH)
    for o in range(1, nt):
        pl.semaphore_signal(barrier, inc=1, device_id=dev(a, w, lax.rem(t + o, nt)), device_id_type=MESH)
    pl.semaphore_wait(barrier, na + nw + nt - 3)

    def a_copy(src, b, s, dr, h):
        return copy(src, abuf.at[b, h], a_send.at[dr, s, h], a_recv.at[dr, s + 1, h],
                    dev(a - (2 * dr - 1), w, t))

    for h in range(CHUNKS):
        for dr in range(2):
            target = a - (2 * dr - 1)

            @pl.when((target >= 0) & (target < na))
            def _():
                a_copy(hid.at[pl.ds(h * half, half), :], a, 0, dr, h).start()
    for o in range(1, nw):
        p = lax.rem(w + o, nw)
        copy(wei, wbuf.at[w], w_send.at[p], w_recv.at[w], dev(a, p, t)).start()
    locals_ = [pltpu.make_async_copy(wei, wbuf.at[w], loc_sem.at[CHUNKS])]
    locals_ += [
        pltpu.make_async_copy(hid.at[pl.ds(h * half, half), :], abuf.at[a, h], loc_sem.at[h])
        for h in range(CHUNKS)
    ]
    for c in locals_:
        c.start()
    for c in locals_:
        c.wait()

    def mm(b, h, slot):
        term = lax.dot_general(
            abuf[b, h], wbuf[slot], (((1,), (1,)), ((), ())),
            preferred_element_type=jnp.float32)
        term = term.astype(pbuf.dtype)
        for k in range(nt):
            pbuf[b, h, k, slot] = term[k * rr:(k + 1) * rr]

    def mm_whole(b, slot):
        rows = abuf[b].reshape(CHUNKS * half, abuf.shape[-1])
        term = lax.dot_general(
            rows, wbuf[slot], (((1,), (1,)), ((), ())), preferred_element_type=jnp.float32)
        term = term.astype(pbuf.dtype)
        for h in range(CHUNKS):
            for k in range(nt):
                first = h * half + k * rr
                pbuf[b, h, k, slot] = term[first:first + rr]

    def p_copy(b, h, slot, peer, me):
        return copy(pbuf.at[b, h, peer, slot], rbuf.at[b, h, me, slot],
                    p_send.at[b, h, peer, slot], p_recv.at[b, h, me, slot], dev(a, w, peer))

    def s_copy(b, h, slot, src):
        return copy(sbuf.at[b, h, slot], srec.at[src, h, slot], s_send.at[b, h, slot],
                    s_recv.at[src, h, slot], dev(b, w, t))

    def g_copy(src, h, slot, peer, me):
        return copy(srec.at[src, h, slot], gbuf.at[src, h, me, slot],
                    g_send.at[src, h, peer, slot], g_recv.at[src, h, me, slot], dev(a, w, peer))

    def send_terms(b, h, slot):
        for o in range(1, nt):
            p_copy(b, h, slot, lax.rem(t + o, nt), t).start()

    def add_terms(b, h, slot):
        total = pbuf[b, h, t, slot].astype(jnp.float32)
        for o in range(1, nt):
            peer = lax.rem(t + o, nt)
            p_copy(b, h, slot, peer, peer).wait_recv()
            total = total + rbuf[b, h, peer, slot].astype(jnp.float32)
        total = total.astype(sbuf.dtype)

        @pl.when(b == a)
        def _():
            srec[b, h, slot] = total

        @pl.when(b != a)
        def _():
            sbuf[b, h, slot] = total
            s_copy(b, h, slot, a).start()

    def spread(src, h, slot):
        @pl.when(src != a)
        def _():
            s_copy(src, h, slot, src).wait_recv()

        for o in range(1, nt):
            g_copy(src, h, slot, lax.rem(t + o, nt), t).start()

    def loop(n, body):
        lax.fori_loop(0, n, lambda i, c: (body(i), c)[1], 0)

    def own(h):
        mm(a, h, w)
        send_terms(a, h, w)
        add_terms(a, h, w)

    loop(CHUNKS, own)

    def arrive(b, s, dr, h):
        a_copy(abuf.at[b, h], b, s - 1, dr, h).wait_recv()
        target = a - (2 * dr - 1)

        @pl.when((target >= 0) & (target < na))
        def _():
            a_copy(abuf.at[b, h], b, s, dr, h).start()

    def step(i):
        dr = lax.rem(i, 2)
        h = lax.rem(lax.div(i, 2), CHUNKS)
        s = lax.div(i, 2 * CHUNKS) + 1
        b = a + (2 * dr - 1) * s

        @pl.when((b >= 0) & (b < na))
        def _():
            arrive(b, s, dr, h)
            mm(b, h, w)
            send_terms(b, h, w)
            add_terms(b, h, w)

    loop((na - 2) * 2 * CHUNKS, step)

    def near(i, body):
        b, h = lax.div(i, CHUNKS), lax.rem(i, CHUNKS)

        @pl.when((b - a <= na - 2) & (a - b <= na - 2))
        def _():
            body(b, h)


    for o in range(1, nw):
        p = lax.rem(w + o, nw)
        copy(wei, wbuf.at[p], w_send.at[p], w_recv.at[p], dev(a, p, t)).wait_recv()

    def each_other(body):
        return lambda b, h: loop(nw - 1, lambda o: body(b, h, lax.rem(w + 1 + o, nw)))

    def multiply(b, h, slot):
        mm(b, h, slot)
        send_terms(b, h, slot)

    def multiply_whole(b):
        @pl.when((b - a <= na - 2) & (a - b <= na - 2))
        def _():
            def one(o):
                slot = lax.rem(w + 1 + o, nw)
                mm_whole(b, slot)
                loop(CHUNKS, lambda h: send_terms(b, h, slot))

            loop(nw - 1, one)

    def late(h):
        far = na - 1 - a
        arrive(far, na - 1, jnp.where(a == 0, 1, 0), h)
        loop(nw, lambda slot: multiply(far, h, slot))
        loop(nw, lambda slot: add_terms(far, h, slot))

    end = (a == 0) | (a == na - 1)
    loop(na, multiply_whole)
    loop(na * CHUNKS, lambda i: near(i, each_other(add_terms)))
    loop(na * CHUNKS, lambda i: near(i, lambda b, h: spread(b, h, w)))
    pl.when(end)(lambda: loop(CHUNKS - 1, late))

    def prompt(b, h):
        pl.when((b - a != 1) & (a - b != 1))(lambda: each_other(spread)(b, h))

    def queued(b, h):
        pl.when((b - a == 1) | (a - b == 1))(lambda: each_other(spread)(b, h))

    def far_spread(h):
        loop(nw, lambda slot: spread(na - 1 - a, h, slot))

    loop(na * CHUNKS, lambda i: near(i, prompt))

    @pl.when(end)
    def _():
        loop(CHUNKS - 1, far_spread)
        late(CHUNKS - 1)

    loop(na * CHUNKS, lambda i: near(i, queued))
    pl.when(end)(lambda: far_spread(CHUNKS - 1))

    def collect(i):
        b, h = lax.div(i, CHUNKS), lax.rem(i, CHUNKS)
        for o in range(1, nt):
            peer = lax.rem(t + o, nt)
            for slot in range(nw):
                g_copy(b, h, slot, peer, peer).wait_recv()
            out[b, h, peer] = gbuf[b, h, peer]
        out[b, h, t] = srec[b, h]

    loop(na * CHUNKS, collect)

    def drain(i):
        b, h = lax.div(i, CHUNKS), lax.rem(i, CHUNKS)
        for slot in range(nw):
            for o in range(1, nt):
                peer = lax.rem(t + o, nt)
                p_copy(b, h, slot, peer, t).wait_send()
                g_copy(b, h, slot, peer, t).wait_send()

            @pl.when(b != a)
            def _():
                s_copy(b, h, slot, a).wait_send()

    loop(na * CHUNKS, drain)

    def drain_a(i):
        dr = lax.rem(i, 2)
        h = lax.rem(lax.div(i, 2), CHUNKS)
        s = lax.div(i, 2 * CHUNKS)
        b = a + (2 * dr - 1) * s
        target = a - (2 * dr - 1)

        @pl.when((b >= 0) & (b < na) & (target >= 0) & (target < na))
        def _():
            a_copy(abuf.at[b, h], b, s, dr, h).wait_send()

    loop((na - 1) * 2 * CHUNKS, drain_a)
    for o in range(1, nw):
        p = lax.rem(w + o, nw)
        copy(wei, wbuf.at[w], w_send.at[p], w_recv.at[w], dev(a, p, t)).wait_send()


def peak_kernel(n, x, out, got, ss, rs):
    d = lax.axis_index("dp")
    t = lax.axis_index("tensor")
    barrier = pltpu.get_barrier_semaphore()
    for o in range(1, n):
        pl.semaphore_signal(barrier, inc=1, device_id=(lax.rem(d + o, n), t), device_id_type=MESH)
    pl.semaphore_wait(barrier, n - 1)

    def copy(o, slot):
        return pltpu.make_async_remote_copy(
            src_ref=x, dst_ref=got.at[slot], send_sem=ss.at[o], recv_sem=rs.at[slot],
            device_id=(lax.rem(d + o, n), t), device_id_type=MESH)

    for o in range(1, n):
        copy(o, o).start()
    best = x[...]
    for o in range(1, n):
        copy(o, o).wait_recv()
        best = jnp.maximum(best, got[o])
    out[...] = best
    for o in range(1, n):
        copy(o, o).wait_send()


def history_kernel(x, hist, peaks, history, scales):
    kept = hist[...]
    best = x[:kept.shape[0], :1]
    lane = lax.broadcasted_iota(jnp.int32, kept.shape, 1)
    new = jnp.where(lane == 0, best, pltpu.roll(kept, 1, 1))
    history[...] = new
    scale = float_limit / jnp.maximum(jnp.max(new, axis=1, keepdims=True), 1.0)
    for i in range(kept.shape[0]):
        peaks[i] = best[i, 0]
        scales[i] = scale[i, 0]


def all_max(values, hist, n):
    vmem = pl.BlockSpec(memory_space=pltpu.VMEM)
    smem = pl.BlockSpec(memory_space=pltpu.SMEM)
    best = pl.pallas_call(
        functools.partial(peak_kernel, n),
        out_shape=jax.ShapeDtypeStruct(values.shape, values.dtype),
        in_specs=[vmem],
        out_specs=vmem,
        scratch_shapes=[
            pltpu.VMEM((n,) + values.shape, values.dtype),
            pltpu.SemaphoreType.DMA((n,)),
            pltpu.SemaphoreType.DMA((n,)),
        ],
        compiler_params=pltpu.CompilerParams(collective_id=1, has_side_effects=True),
    )(values)
    column = jax.ShapeDtypeStruct((hist.shape[0],), jnp.float32)
    return pl.pallas_call(
        history_kernel,
        out_shape=(column, jax.ShapeDtypeStruct(hist.shape, hist.dtype), column),
        in_specs=[vmem] * 2,
        out_specs=[smem, vmem, smem],
    )(best, hist)


def finish_kernel(dims, scale, parts, residual, post_gain, pre_gain, cast_out, stream_out, peaks, summed):
    (na, sa), (nw, sw), cols = dims
    for a in range(na):
        for w in range(nw):
            first = (a * sa + w * sw) * cols
            summed[:, first:first + cols] = parts[a, 0, 0, w].astype(jnp.float32)
    x = summed[...]
    stream = residual[...].astype(jnp.float32) + rms_norm(x, post_gain[...].reshape(1, -1))
    normed = rms_norm(stream, pre_gain[...].reshape(1, -1))
    s = scale[0]
    cast_out[...] = (jnp.clip(normed * s, -float_limit, float_limit) / s).astype(cast_out.dtype)
    stream_out[...] = stream.astype(stream_out.dtype)
    row = lax.broadcasted_iota(jnp.int32, peaks.shape, 0)
    tops = [jnp.max(jnp.abs(v)) for v in (x, stream, normed)]
    tile = jnp.where(row == 0, tops[0], jnp.where(row == 1, tops[1], tops[2]))
    first_step = (pl.program_id(0) == 0) & (pl.program_id(1) == 0)

    @pl.when(first_step)
    def _():
        peaks[...] = tile

    @pl.when(jnp.logical_not(first_step))
    def _():
        peaks[...] = jnp.maximum(peaks[...], tile)


def finish(parts, residual, post_gain, pre_gain, cast_scale, long, short):
    na, chunks, nt, nw, rr, cols = parts.shape
    width = residual.shape[1]
    rows = pl.BlockSpec((rr, width), lambda h, k: (h * nt + k, 0))
    gain = pl.BlockSpec((width,), lambda h, k: (0,))
    kind = jax.ShapeDtypeStruct(residual.shape, jnp.bfloat16)
    return pl.pallas_call(
        functools.partial(finish_kernel, (long, short, cols)),
        grid=(chunks, nt),
        out_shape=(kind, kind, jax.ShapeDtypeStruct((8, 128), jnp.float32)),
        in_specs=[
            pl.BlockSpec(memory_space=pltpu.SMEM),
            pl.BlockSpec((na, 1, 1, nw, rr, cols), lambda h, k: (0, h, k, 0, 0, 0)),
            rows, gain, gain,
        ],
        out_specs=[rows, rows, pl.BlockSpec((8, 128), lambda h, k: (0, 0))],
        scratch_shapes=[pltpu.VMEM((rr, width), jnp.float32)],
    )(cast_scale, parts, residual, post_gain, pre_gain)


def project(hidden, down_weight, long, short, nt):
    rows, depth = hidden.shape
    cols = down_weight.shape[0]
    na, nw = long[0], short[0]
    half = rows // CHUNKS
    rr = half // nt
    kind = hidden.dtype
    dma = pltpu.SemaphoreType.DMA
    return pl.pallas_call(
        functools.partial(project_kernel, (long, short, nt, half, rr)),
        out_shape=jax.ShapeDtypeStruct((na, CHUNKS, nt, nw, rr, cols), kind),
        in_specs=[pl.BlockSpec(memory_space=pl.ANY)] * 2,
        out_specs=pl.BlockSpec(memory_space=pltpu.VMEM),
        scratch_shapes=[
            pltpu.VMEM((na, CHUNKS, half, depth), kind),
            pltpu.VMEM((nw, cols, depth), kind),
            pltpu.VMEM((na, CHUNKS, nt, nw, rr, cols), kind),
            pltpu.VMEM((na, CHUNKS, nt, nw, rr, cols), kind),
            pltpu.VMEM((na, CHUNKS, nw, rr, cols), kind),
            pltpu.VMEM((na, CHUNKS, nw, rr, cols), kind),
            pltpu.VMEM((na, CHUNKS, nt, nw, rr, cols), kind),
            dma((CHUNKS + 1,)),
            dma((2, na, CHUNKS)), dma((2, na + 1, CHUNKS)),
            dma((nw,)), dma((nw,)),
            dma((na, CHUNKS, nt, nw)), dma((na, CHUNKS, nt, nw)),
            dma((na, CHUNKS, nw)), dma((na, CHUNKS, nw)),
            dma((na, CHUNKS, nt, nw)), dma((na, CHUNKS, nt, nw)),
        ],
        compiler_params=pltpu.CompilerParams(
            collective_id=0, has_side_effects=True, vmem_limit_bytes=60 * 1024 * 1024),
    )(hidden, down_weight)


def on_device(long, short, nt, hidden, down_weight, residual, post_gain, pre_gain, cast_scale, amax_history):
    parts = project(hidden, down_weight.T, long, short, nt)
    cast_out, stream, tile = finish(parts, residual, post_gain, pre_gain, cast_scale, long, short)
    peaks, new_history, new_scales = all_max(tile, amax_history, long[0] * short[0])
    return (cast_out, stream, peaks, new_history, new_scales)


def solution(mesh):
    long, short = factor(mesh)
    in_specs = (P("dp", "tensor"), P("tensor", "dp"), P("dp", None), P(), P(), P(), P())
    out_specs = (P("dp", None), P("dp", None), P(), P(), P())
    return jax.shard_map(
        functools.partial(on_device, long, short, mesh.shape["tensor"]),
        mesh=mesh, in_specs=in_specs, out_specs=out_specs, check_vma=False
    )
```

```python
import functools

import jax
import jax.numpy as jnp
from jax import lax
from jax.experimental import pallas as pl
from jax.experimental.pallas import tpu as pltpu
from jax.sharding import PartitionSpec as P

MESH = pl.DeviceIdType.MESH
norm_epsilon = 1e-06
float_limit = 448.0
CHUNKS = 2


def rms_norm(values, gain_vector):
    return (
        values
        * lax.rsqrt(jnp.mean(values * values, axis=-1, keepdims=True) + norm_epsilon)
        * gain_vector
    )


def factor(mesh):
    devices = mesh.devices
    count = devices.shape[0]
    coords = [tuple(devices[i, 0].coords) for i in range(count)]
    inner = 1
    if count > 1:
        axis = [p != q for p, q in zip(coords[0], coords[1])].index(True)
        while inner < count and all(
            p == q for k, (p, q) in enumerate(zip(coords[0], coords[inner])) if k != axis
        ):
            inner += 1
    outer = count // inner
    if outer >= inner:
        return (outer, inner), (inner, 1)
    return (inner, 1), (outer, inner)


def project_kernel(dims, hid, wei, out, abuf, wbuf, pbuf, rbuf, sbuf, srec, gbuf,
                   loc_sem, a_send, a_recv, w_send, w_recv, p_send, p_recv,
                   s_send, s_recv, g_send, g_recv):
    (na, sa), (nw, sw), nt, half, rr = dims
    d = lax.axis_index("dp")
    t = lax.axis_index("tensor")
    a = lax.rem(lax.div(d, sa), na)
    w = lax.rem(lax.div(d, sw), nw)

    def dev(a_, w_, t_):
        return (a_ * sa + w_ * sw, t_)

    def copy(src, dst, ss, rs, to):
        return pltpu.make_async_remote_copy(
            src_ref=src, dst_ref=dst, send_sem=ss, recv_sem=rs,
            device_id=to, device_id_type=MESH)

    barrier = pltpu.get_barrier_semaphore()
    for o in range(1, na):
        pl.semaphore_signal(barrier, inc=1, device_id=dev(lax.rem(a + o, na), w, t), device_id_type=MESH)
    for o in range(1, nw):
        pl.semaphore_signal(barrier, inc=1, device_id=dev(a, lax.rem(w + o, nw), t), device_id_type=MESH)
    for o in range(1, nt):
        pl.semaphore_signal(barrier, inc=1, device_id=dev(a, w, lax.rem(t + o, nt)), device_id_type=MESH)
    pl.semaphore_wait(barrier, na + nw + nt - 3)

    def a_copy(src, b, s, dr, h):
        return copy(src, abuf.at[b, h], a_send.at[dr, s, h], a_recv.at[dr, s + 1, h],
                    dev(a - (2 * dr - 1), w, t))

    for h in range(CHUNKS):
        for dr in range(2):
            target = a - (2 * dr - 1)

            @pl.when((target >= 0) & (target < na))
            def _():
                a_copy(hid.at[pl.ds(h * half, half), :], a, 0, dr, h).start()
    for o in range(1, nw):
        p = lax.rem(w + o, nw)
        copy(wei, wbuf.at[w], w_send.at[p], w_recv.at[w], dev(a, p, t)).start()
    locals_ = [pltpu.make_async_copy(wei, wbuf.at[w], loc_sem.at[CHUNKS])]
    locals_ += [
        pltpu.make_async_copy(hid.at[pl.ds(h * half, half), :], abuf.at[a, h], loc_sem.at[h])
        for h in range(CHUNKS)
    ]
    for c in locals_:
        c.start()
    for c in locals_:
        c.wait()

    def mm(b, h, slot):
        term = lax.dot_general(
            abuf[b, h], wbuf[slot], (((1,), (1,)), ((), ())),
            preferred_element_type=jnp.float32)
        term = term.astype(pbuf.dtype)
        for k in range(nt):
            pbuf[b, h, k, slot] = term[k * rr:(k + 1) * rr]

    def mm_whole(b, slot):
        rows = abuf[b].reshape(CHUNKS * half, abuf.shape[-1])
        term = lax.dot_general(
            rows, wbuf[slot], (((1,), (1,)), ((), ())), preferred_element_type=jnp.float32)
        term = term.astype(pbuf.dtype)
        for h in range(CHUNKS):
            for k in range(nt):
                first = h * half + k * rr
                pbuf[b, h, k, slot] = term[first:first + rr]

    def p_copy(b, h, slot, peer, me):
        return copy(pbuf.at[b, h, peer, slot], rbuf.at[b, h, me, slot],
                    p_send.at[b, h, peer, slot], p_recv.at[b, h, me, slot], dev(a, w, peer))

    def s_copy(b, h, slot, src):
        return copy(sbuf.at[b, h, slot], srec.at[src, h, slot], s_send.at[b, h, slot],
                    s_recv.at[src, h, slot], dev(b, w, t))

    def g_copy(src, h, slot, peer, me):
        return copy(srec.at[src, h, slot], gbuf.at[src, h, me, slot],
                    g_send.at[src, h, peer, slot], g_recv.at[src, h, me, slot], dev(a, w, peer))

    def send_terms(b, h, slot):
        for o in range(1, nt):
            p_copy(b, h, slot, lax.rem(t + o, nt), t).start()

    def add_terms(b, h, slot):
        total = pbuf[b, h, t, slot].astype(jnp.float32)
        for o in range(1, nt):
            peer = lax.rem(t + o, nt)
            p_copy(b, h, slot, peer, peer).wait_recv()
            total = total + rbuf[b, h, peer, slot].astype(jnp.float32)
        total = total.astype(sbuf.dtype)

        @pl.when(b == a)
        def _():
            srec[b, h, slot] = total

        @pl.when(b != a)
        def _():
            sbuf[b, h, slot] = total
            s_copy(b, h, slot, a).start()

    def spread(src, h, slot):
        @pl.when(src != a)
        def _():
            s_copy(src, h, slot, src).wait_recv()

        for o in range(1, nt):
            g_copy(src, h, slot, lax.rem(t + o, nt), t).start()

    def loop(n, body):
        lax.fori_loop(0, n, lambda i, c: (body(i), c)[1], 0)

    def own(h):
        mm(a, h, w)
        send_terms(a, h, w)
        add_terms(a, h, w)

    loop(CHUNKS, own)

    def arrive(b, s, dr, h):
        a_copy(abuf.at[b, h], b, s - 1, dr, h).wait_recv()
        target = a - (2 * dr - 1)

        @pl.when((target >= 0) & (target < na))
        def _():
            a_copy(abuf.at[b, h], b, s, dr, h).start()

    def step(i):
        dr = lax.rem(i, 2)
        h = lax.rem(lax.div(i, 2), CHUNKS)
        s = lax.div(i, 2 * CHUNKS) + 1
        b = a + (2 * dr - 1) * s

        @pl.when((b >= 0) & (b < na))
        def _():
            arrive(b, s, dr, h)
            mm(b, h, w)
            send_terms(b, h, w)
            add_terms(b, h, w)

    loop((na - 2) * 2 * CHUNKS, step)

    def near(i, body):
        b, h = lax.div(i, CHUNKS), lax.rem(i, CHUNKS)

        @pl.when((b - a <= na - 2) & (a - b <= na - 2))
        def _():
            body(b, h)


    for o in range(1, nw):
        p = lax.rem(w + o, nw)
        copy(wei, wbuf.at[p], w_send.at[p], w_recv.at[p], dev(a, p, t)).wait_recv()

    def each_other(body):
        return lambda b, h: loop(nw - 1, lambda o: body(b, h, lax.rem(w + 1 + o, nw)))

    def multiply(b, h, slot):
        mm(b, h, slot)
        send_terms(b, h, slot)

    def multiply_whole(b):
        @pl.when((b - a <= na - 2) & (a - b <= na - 2))
        def _():
            def one(o):
                slot = lax.rem(w + 1 + o, nw)
                mm_whole(b, slot)
                loop(CHUNKS, lambda h: send_terms(b, h, slot))

            loop(nw - 1, one)

    def late(h):
        far = na - 1 - a
        arrive(far, na - 1, jnp.where(a == 0, 1, 0), h)
        loop(nw, lambda slot: multiply(far, h, slot))
        loop(nw, lambda slot: add_terms(far, h, slot))

    end = (a == 0) | (a == na - 1)
    loop(na, multiply_whole)
    loop(na * CHUNKS, lambda i: near(i, each_other(add_terms)))
    loop(na * CHUNKS, lambda i: near(i, lambda b, h: spread(b, h, w)))
    pl.when(end)(lambda: loop(CHUNKS - 1, late))

    def prompt(b, h):
        pl.when((b - a != 1) & (a - b != 1))(lambda: each_other(spread)(b, h))

    def queued(b, h):
        pl.when((b - a == 1) | (a - b == 1))(lambda: each_other(spread)(b, h))

    def far_spread(h):
        loop(nw, lambda slot: spread(na - 1 - a, h, slot))

    loop(na * CHUNKS, lambda i: near(i, prompt))

    @pl.when(end)
    def _():
        loop(CHUNKS - 1, far_spread)
        late(CHUNKS - 1)

    loop(na * CHUNKS, lambda i: near(i, queued))
    pl.when(end)(lambda: far_spread(CHUNKS - 1))

    def collect(i):
        b, h = lax.div(i, CHUNKS), lax.rem(i, CHUNKS)
        for o in range(1, nt):
            peer = lax.rem(t + o, nt)
            for slot in range(nw):
                g_copy(b, h, slot, peer, peer).wait_recv()
            out[b, h, peer] = gbuf[b, h, peer]
        out[b, h, t] = srec[b, h]

    loop(na * CHUNKS, collect)

    def drain(i):
        b, h = lax.div(i, CHUNKS), lax.rem(i, CHUNKS)
        for slot in range(nw):
            for o in range(1, nt):
                peer = lax.rem(t + o, nt)
                p_copy(b, h, slot, peer, t).wait_send()
                g_copy(b, h, slot, peer, t).wait_send()

            @pl.when(b != a)
            def _():
                s_copy(b, h, slot, a).wait_send()

    loop(na * CHUNKS, drain)

    def drain_a(i):
        dr = lax.rem(i, 2)
        h = lax.rem(lax.div(i, 2), CHUNKS)
        s = lax.div(i, 2 * CHUNKS)
        b = a + (2 * dr - 1) * s
        target = a - (2 * dr - 1)

        @pl.when((b >= 0) & (b < na) & (target >= 0) & (target < na))
        def _():
            a_copy(abuf.at[b, h], b, s, dr, h).wait_send()

    loop((na - 1) * 2 * CHUNKS, drain_a)
    for o in range(1, nw):
        p = lax.rem(w + o, nw)
        copy(wei, wbuf.at[w], w_send.at[p], w_recv.at[w], dev(a, p, t)).wait_send()


def peak_kernel(n, x, out, got, ss, rs):
    d = lax.axis_index("dp")
    t = lax.axis_index("tensor")
    barrier = pltpu.get_barrier_semaphore()
    for o in range(1, n):
        pl.semaphore_signal(barrier, inc=1, device_id=(lax.rem(d + o, n), t), device_id_type=MESH)
    pl.semaphore_wait(barrier, n - 1)

    def copy(o, slot):
        return pltpu.make_async_remote_copy(
            src_ref=x, dst_ref=got.at[slot], send_sem=ss.at[o], recv_sem=rs.at[slot],
            device_id=(lax.rem(d + o, n), t), device_id_type=MESH)

    for o in range(1, n):
        copy(o, o).start()
    best = x[...]
    for o in range(1, n):
        copy(o, o).wait_recv()
        best = jnp.maximum(best, got[o])
    out[...] = best
    for o in range(1, n):
        copy(o, o).wait_send()


def history_kernel(x, hist, peaks, history, scales):
    kept = hist[...]
    best = x[:kept.shape[0], :1]
    lane = lax.broadcasted_iota(jnp.int32, kept.shape, 1)
    new = jnp.where(lane == 0, best, pltpu.roll(kept, 1, 1))
    history[...] = new
    scale = float_limit / jnp.maximum(jnp.max(new, axis=1, keepdims=True), 1.0)
    for i in range(kept.shape[0]):
        peaks[i] = best[i, 0]
        scales[i] = scale[i, 0]


def all_max(values, hist, n):
    vmem = pl.BlockSpec(memory_space=pltpu.VMEM)
    smem = pl.BlockSpec(memory_space=pltpu.SMEM)
    best = pl.pallas_call(
        functools.partial(peak_kernel, n),
        out_shape=jax.ShapeDtypeStruct(values.shape, values.dtype),
        in_specs=[vmem],
        out_specs=vmem,
        scratch_shapes=[
            pltpu.VMEM((n,) + values.shape, values.dtype),
            pltpu.SemaphoreType.DMA((n,)),
            pltpu.SemaphoreType.DMA((n,)),
        ],
        compiler_params=pltpu.CompilerParams(collective_id=1, has_side_effects=True),
    )(values)
    column = jax.ShapeDtypeStruct((hist.shape[0],), jnp.float32)
    return pl.pallas_call(
        history_kernel,
        out_shape=(column, jax.ShapeDtypeStruct(hist.shape, hist.dtype), column),
        in_specs=[vmem] * 2,
        out_specs=[smem, vmem, smem],
    )(best, hist)


def finish_kernel(dims, scale, parts, residual, post_gain, pre_gain, cast_out, stream_out, peaks, summed, tops):
    (na, sa), (nw, sw), cols = dims
    for a in range(na):
        for w in range(nw):
            first = (a * sa + w * sw) * cols
            summed[:, first:first + cols] = parts[a, 0, 0, w].astype(jnp.float32)
    x = summed[...]
    stream = residual[...].astype(jnp.float32) + rms_norm(x, post_gain[...].reshape(1, -1))
    normed = rms_norm(stream, pre_gain[...].reshape(1, -1))
    s = scale[0]
    inverse = 1.0 / jnp.full((1, 1), s, jnp.float32)
    cast_out[...] = (jnp.clip(normed * s, -float_limit, float_limit) * inverse).astype(cast_out.dtype)
    stream_out[...] = stream.astype(stream_out.dtype)
    first_step = (pl.program_id(0) == 0) & (pl.program_id(1) == 0)
    last_step = (pl.program_id(0) == pl.num_programs(0) - 1) & (
        pl.program_id(1) == pl.num_programs(1) - 1)

    @pl.when(first_step)
    def _():
        tops[...] = jnp.zeros_like(tops)

    for i, v in enumerate((x, stream, normed)):
        most = jnp.max(jnp.abs(v).reshape(-1, 8, v.shape[1]), axis=0)
        tops[i] = jnp.maximum(tops[i], most)

    @pl.when(last_step)
    def _():
        row = lax.broadcasted_iota(jnp.int32, peaks.shape, 0)
        best = [jnp.max(tops[i]) for i in range(3)]
        peaks[...] = jnp.where(row == 0, best[0], jnp.where(row == 1, best[1], best[2]))


def finish(parts, residual, post_gain, pre_gain, cast_scale, long, short):
    na, chunks, nt, nw, rr, cols = parts.shape
    width = residual.shape[1]
    rows = pl.BlockSpec((rr, width), lambda h, k: (h * nt + k, 0))
    gain = pl.BlockSpec((width,), lambda h, k: (0,))
    kind = jax.ShapeDtypeStruct(residual.shape, jnp.bfloat16)
    return pl.pallas_call(
        functools.partial(finish_kernel, (long, short, cols)),
        grid=(chunks, nt),
        out_shape=(kind, kind, jax.ShapeDtypeStruct((8, 128), jnp.float32)),
        in_specs=[
            pl.BlockSpec(memory_space=pltpu.SMEM),
            pl.BlockSpec((na, 1, 1, nw, rr, cols), lambda h, k: (0, h, k, 0, 0, 0)),
            rows, gain, gain,
        ],
        out_specs=[rows, rows, pl.BlockSpec((8, 128), lambda h, k: (0, 0))],
        scratch_shapes=[
            pltpu.VMEM((rr, width), jnp.float32),
            pltpu.VMEM((3, 8, width), jnp.float32),
        ],
    )(cast_scale, parts, residual, post_gain, pre_gain)


def project(hidden, down_weight, long, short, nt):
    rows, depth = hidden.shape
    cols = down_weight.shape[0]
    na, nw = long[0], short[0]
    half = rows // CHUNKS
    rr = half // nt
    kind = hidden.dtype
    dma = pltpu.SemaphoreType.DMA
    return pl.pallas_call(
        functools.partial(project_kernel, (long, short, nt, half, rr)),
        out_shape=jax.ShapeDtypeStruct((na, CHUNKS, nt, nw, rr, cols), kind),
        in_specs=[pl.BlockSpec(memory_space=pl.ANY)] * 2,
        out_specs=pl.BlockSpec(memory_space=pltpu.VMEM),
        scratch_shapes=[
            pltpu.VMEM((na, CHUNKS, half, depth), kind),
            pltpu.VMEM((nw, cols, depth), kind),
            pltpu.VMEM((na, CHUNKS, nt, nw, rr, cols), kind),
            pltpu.VMEM((na, CHUNKS, nt, nw, rr, cols), kind),
            pltpu.VMEM((na, CHUNKS, nw, rr, cols), kind),
            pltpu.VMEM((na, CHUNKS, nw, rr, cols), kind),
            pltpu.VMEM((na, CHUNKS, nt, nw, rr, cols), kind),
            dma((CHUNKS + 1,)),
            dma((2, na, CHUNKS)), dma((2, na + 1, CHUNKS)),
            dma((nw,)), dma((nw,)),
            dma((na, CHUNKS, nt, nw)), dma((na, CHUNKS, nt, nw)),
            dma((na, CHUNKS, nw)), dma((na, CHUNKS, nw)),
            dma((na, CHUNKS, nt, nw)), dma((na, CHUNKS, nt, nw)),
        ],
        compiler_params=pltpu.CompilerParams(
            collective_id=0, has_side_effects=True, vmem_limit_bytes=60 * 1024 * 1024),
    )(hidden, down_weight)


def on_device(long, short, nt, hidden, down_weight, residual, post_gain, pre_gain, cast_scale, amax_history):
    parts = project(hidden, down_weight.T, long, short, nt)
    cast_out, stream, tile = finish(parts, residual, post_gain, pre_gain, cast_scale, long, short)
    peaks, new_history, new_scales = all_max(tile, amax_history, long[0] * short[0])
    return (cast_out, stream, peaks, new_history, new_scales)


def solution(mesh):
    long, short = factor(mesh)
    in_specs = (P("dp", "tensor"), P("tensor", "dp"), P("dp", None), P(), P(), P(), P())
    out_specs = (P("dp", None), P("dp", None), P(), P(), P())
    return jax.shard_map(
        functools.partial(on_device, long, short, mesh.shape["tensor"]),
        mesh=mesh, in_specs=in_specs, out_specs=out_specs, check_vma=False
    )
```
